32 devices in a mesh: dp: 4 (over y, x), vocab: 8 (over z, core).
Axes of the slice: x: 2, y: 2, z: 4, core: 2. Of those that a mesh axis runs over, the one named last changes fastest.
Arguments:
- hidden: bfloat16 [512, 8192], P('dp', 'vocab'), may hold values from -20 to 20
- weight: bfloat16 [8192, 4752], P('dp', 'vocab'), may hold values from -0.198873782 to 0.198873782
- targets: int32 [512], P('dp'), may hold values from 0 to 4751
- loss_mask: int32 [512], P('dp'), may hold values 0 or 1
Outputs:
- grad_hidden: bfloat16 [512, 8192], P('dp', 'vocab')
- grad_weight: bfloat16 [8192, 4752], P('dp', 'vocab')
- token_loss: float32 [512], P('dp')
- grad_norm: float32 [], replicated
The draws below stay inside these ranges and needn't reach their ends.
All inputs are finite; a program needn't handle non-finite values. No bound on the sum of `loss_mask` on one device may be relied on, other than what follows from the above.
Results may differ from the reference program's by a relative error of at most 0.0034.
Values may be sent and summed in bfloat16 or wider, within the bound.
A program may use at most 128 MiB of HBM per device.

```python
import math
import jax
import jax.numpy as jnp
import numpy as np
from jax import lax

D = 8192
V_DEV = 594
VOCAB = 4752
TOKENS = 512
N_VOCAB = 8


def weight_column(key, column):
    column_key = jax.random.fold_in(jax.random.fold_in(key, 71), column)
    values = jnp.clip(jax.random.normal(column_key, (D,), jnp.float32), -6.0, 6.0)
    return values * (3.0 / math.sqrt(D))


def draw_weight(key, part):
    columns = jax.vmap(lambda column: weight_column(key, column))(jnp.arange(VOCAB, dtype=jnp.int32))
    return columns.T.astype(jnp.bfloat16)


def draw_hidden(key, part):
    drawn = jnp.clip(jax.random.normal(jax.random.fold_in(key, 13), (TOKENS, D), jnp.float32), -6.0, 6.0)
    return drawn.astype(jnp.bfloat16)


def set_ends(array, own_key, least, largest):
    longest = array.shape.index(max(array.shape))
    spots = []
    for shift in (0, 1):
        where = [jax.random.randint(jax.random.fold_in(own_key, axis), (), 0, length) for axis, length in enumerate(array.shape)]
        where[longest] = (where[longest] + shift) % array.shape[longest]
        spots.append(tuple(where))
    return array.at[spots[0]].set(least).at[spots[1]].set(largest)


def rank_table(number_of, lean):
    weights = [(1 << 20) // math.isqrt(rank ** lean) + 1 for rank in range(1, number_of + 1)]
    deviation = 1 + sum(weights) // (1 << 30)
    return np.cumsum(np.array([max(1, weight // deviation) for weight in weights]))


def ranked_ids(stream_key, shape, number_of, lean):
    listing = rank_table(number_of, lean)
    lot = jax.random.randint(jax.random.fold_in(stream_key, 1), shape, 0, int(listing[number_of - 1]))
    rank = jnp.searchsorted(jnp.asarray(listing, jnp.int32), lot, side="right")
    return jax.random.permutation(jax.random.fold_in(stream_key, 2), number_of)[rank].astype(jnp.int32)


def setup_inputs(seed: int = 0) -> dict:
    key_of = jax.random.split(jax.random.key(seed), 5)
    hidden = draw_hidden(jax.random.fold_in(key_of[4], 71), 0)
    weight = draw_weight(jax.random.fold_in(key_of[4], 71), 0)
    targets = set_ends(ranked_ids(key_of[2], (TOKENS,), VOCAB, 2), jax.random.fold_in(key_of[2], 3), 0, VOCAB - 1).astype(jnp.int32)
    loss_mask = set_ends((jax.random.randint(key_of[3], (TOKENS,), 0, 4) < 3).astype(jnp.int32), jax.random.fold_in(key_of[3], 1), 0, 1)
    return dict(hidden=hidden, weight=weight, targets=targets, loss_mask=loss_mask)


loss_scale = 16.0

def reference(hidden, weight, targets, loss_mask):
    logits = jnp.dot(hidden, weight, preferred_element_type=jnp.float32)
    row_top = lax.optimization_barrier(jnp.max(logits, axis=1, keepdims=True))
    log_total = row_top[:, 0] + jnp.log(lax.optimization_barrier(jnp.sum(jnp.exp(logits - row_top), axis=1)))
    onehot = (lax.broadcasted_iota(jnp.int32, logits.shape, 1) == targets[:, None]).astype(jnp.float32)
    target_logit = lax.optimization_barrier(jnp.sum(logits * onehot, axis=1))
    row_keep = loss_mask.astype(jnp.float32)
    token_loss = row_keep * (log_total - target_logit)
    softmax = jnp.exp(logits - log_total[:, None])
    dlogits = (loss_scale * row_keep[:, None] * (softmax - onehot)).astype(jnp.bfloat16)
    hidden_grad_full = lax.dot_general(dlogits, weight, (((1,), (1,)), ((), ())), preferred_element_type=jnp.float32)

    def weight_block(block_index):
        block_start = (block_index * V_DEV).astype(jnp.int32)
        grad_slice = lax.dynamic_slice_in_dim(dlogits, block_start, V_DEV, 1)
        grad_piece = lax.dot_general(hidden, grad_slice, (((0,), (0,)), ((), ())), preferred_element_type=jnp.float32)
        return (grad_piece.astype(jnp.bfloat16), jnp.sum(grad_piece * grad_piece))
    blocks, squares = lax.map(weight_block, jnp.arange(N_VOCAB, dtype=jnp.int32))
    grad_weight = jnp.transpose(blocks, (1, 0, 2)).reshape(D, V_DEV * N_VOCAB)
    grad_norm = jnp.sqrt(jnp.sum(squares) + jnp.sum(hidden_grad_full * hidden_grad_full))
    return (hidden_grad_full.astype(jnp.bfloat16), grad_weight, token_loss, grad_norm)
```

```python
import functools

import jax
import jax.numpy as jnp
from jax import lax
from jax.experimental import pallas as pl
from jax.experimental.pallas import tpu as pltpu
from jax.sharding import PartitionSpec as P

loss_scale = 16.0
MESH = pl.DeviceIdType.MESH
f32 = jnp.float32
bf16 = jnp.bfloat16


def dot_nn(a, b):
    return jnp.dot(a, b, preferred_element_type=f32)


def dot_nt(a, b):
    return lax.dot_general(a, b, (((1,), (1,)), ((), ())), preferred_element_type=f32)


def dot_tn(a, b):
    return lax.dot_general(a, b, (((0,), (0,)), ((), ())), preferred_element_type=f32)


def kernel(
    n, nv, cpc,
    hid, w, tgt, keep,
    hg_out, wg_out, loss_out, norm_out,
    gat, hb, lp, lr, st, sr, dall, ps, pr, gs, g1, g2, n1s, n1, n2s, n2,
    h1_s, h1_r, h2_s, hb_r, h3_s, l_s, l_r, s_s, s_r, d_s, d_r,
    p_s, p_r, g1_s, g1_r, g2_s, g2_r, n1_s, n1_r, n2_s, n2_r,
):
    T, F = hid.shape
    V = w.shape[1]
    bpd = nv // n
    zpd = bpd // cpc
    nz = nv // cpc
    k = lax.axis_index("dp")
    j = lax.axis_index("vocab")
    z, c = j // cpc, j % cpc
    sends = []

    def push(src, dst, ss, rs, dp, vocab):
        copy = pltpu.make_async_remote_copy(
            src_ref=src, dst_ref=dst, send_sem=ss, recv_sem=rs,
            device_id={"dp": dp, "vocab": vocab}, device_id_type=MESH,
        )
        copy.start()
        sends.append((src, ss))

    def local(src, dst, sem):
        pltpu.make_async_copy(src, dst, sem).start()

    def arrived(dst, sem):
        pltpu.make_async_copy(dst, dst, sem).wait()

    def turn(s, base, size):
        return lax.rem(base + s, size)

    row_order = list(range(1, n)) + [0]

    barrier = pltpu.get_barrier_semaphore()
    for s in range(1, nv):
        pl.semaphore_signal(barrier, inc=1, device_id={"dp": k, "vocab": turn(s, j, nv)}, device_id_type=MESH)
    for s in range(1, n):
        pl.semaphore_signal(barrier, inc=1, device_id={"dp": turn(s, k, n), "vocab": j}, device_id_type=MESH)
    pl.semaphore_wait(barrier, nv + n - 2)

    for s in range(1, nz):
        to = turn(s, z, nz)
        push(hid, gat.at[z], h1_s.at[s], h1_r.at[z], k, to * cpc + c)
    local(hid, gat.at[z], h1_r.at[z])

    for s in row_order:
        i = turn(s, k, n)
        for q in range(zpd):
            src = gat.at[i * zpd + q]
            arrived(src, h1_r.at[i * zpd + q])
            bl = q * cpc + c
            if s:
                push(src, hb.at[bl, k], h2_s.at[s, q], hb_r.at[k, bl], i, j)
            else:
                local(src, hb.at[bl, k], hb_r.at[k, bl])

    for s in [0] + list(range(1, n)):
        t = turn(s, k, n)
        for q in range(zpd):
            bl = q * cpc + c
            arrived(hb.at[bl, t], hb_r.at[t, bl])
            for d in range(1, cpc):
                push(hb.at[bl, t], hb.at[bl, t], h3_s.at[s, q, d], hb_r.at[t, bl], k, z * cpc + turn(d, c, cpc))

    for s in row_order:
        t = turn(s, k, n)
        for q in range(zpd):
            for d in range(1, cpc):
                bl = q * cpc + turn(d, c, cpc)
                arrived(hb.at[bl, t], hb_r.at[t, bl])
        total = dot_nn(hb[0, t], w[0:F, :])
        for bl in range(1, bpd):
            total += dot_nn(hb[bl, t], w[bl * F:(bl + 1) * F, :])
        if s:
            lp[s - 1] = total
            push(lp.at[s - 1], lr.at[s - 1], l_s.at[s - 1], l_r.at[s - 1], t, j)
    logits = total
    for s in range(n - 1):
        arrived(lr.at[s], l_r.at[s])
        logits += lr[s]

    def to_column(row):
        return jnp.transpose(jnp.broadcast_to(row, (128, T)))[:, :1]

    target_col = to_column(tgt[...].astype(f32)).astype(jnp.int32) - j * V
    onehot = lax.broadcasted_iota(jnp.int32, (T, V), 1) == target_col
    top = jnp.max(logits, axis=1, keepdims=True)
    part = jnp.sum(jnp.exp(logits - top), axis=1, keepdims=True)
    hit = jnp.sum(jnp.where(onehot, logits, 0.0), axis=1, keepdims=True)
    lane = lax.broadcasted_iota(jnp.int32, (T, 128), 1)
    packed = jnp.where(lane == 0, top, jnp.where(lane == 1, part, hit))
    mine = jnp.transpose(packed)[:8, :]
    st[...] = mine
    sr[j] = mine
    for s in range(1, nv):
        push(st, sr.at[j], s_s.at[s], s_r.at[j], k, turn(s, j, nv))
    for s in range(1, nv):
        frm = turn(s, j, nv)
        arrived(sr.at[frm], s_r.at[frm])
    stats = sr[...]
    tops, parts, hits = stats[:, 0, :], stats[:, 1, :], stats[:, 2, :]
    row_top = jnp.max(tops, axis=0, keepdims=True)
    exp_sum = jnp.sum(parts * jnp.exp(tops - row_top), axis=0, keepdims=True)
    target_logit = jnp.sum(hits, axis=0, keepdims=True)
    log_total = row_top + jnp.log(exp_sum)
    row_keep = keep[...].astype(f32)
    loss_out[...] = row_keep * (log_total - target_logit)

    soft = jnp.exp(logits - to_column(log_total))
    dl = (loss_scale * to_column(row_keep) * (soft - jnp.where(onehot, 1.0, 0.0))).astype(bf16)
    dall[k] = dl
    for s in range(1, n):
        push(dall.at[k], dall.at[k], d_s.at[s], d_r.at[k], turn(s, k, n), j)

    for s in [0] + list(range(1, n)):
        t = turn(s, k, n)
        if s:
            arrived(dall.at[t], d_r.at[t])
        for d in range(1, cpc):
            other = turn(d, c, cpc)
            for q in range(zpd):
                off = pl.multiple_of((q * cpc + other) * F, F)
                ps[s, d - 1, q] = dot_nt(dall[t], w[pl.ds(off, F), :])
            push(ps.at[s, d - 1], pr.at[s, d - 1], p_s.at[s, d - 1], p_r.at[s, d - 1], k, z * cpc + other)
    for s in row_order:
        t = turn(s, k, n)
        for d in range(1, cpc):
            arrived(pr.at[s, d - 1], p_r.at[s, d - 1])
        for q in range(zpd):
            off = pl.multiple_of((q * cpc + c) * F, F)
            part_sum = dot_nt(dall[t], w[pl.ds(off, F), :])
            for d in range(1, cpc):
                part_sum += pr[s, d - 1, q]
            gs[s, q] = part_sum.astype(bf16)
        if s:
            push(gs.at[s], g1.at[k], g1_s.at[s], g1_r.at[k], t, j)
        else:
            local(gs.at[s], g1.at[k], g1_r.at[k])

    grads = dall[...].reshape(n * T, V)
    squares = jnp.zeros((1, V), f32)
    rows = bpd * F
    tile = min(F, 256)
    per = rows // tile // n
    done = 0
    for s in row_order[-1:] + row_order[:-1]:
        def step(m, acc):
            first = m * tile
            bl = first // F
            col = pl.multiple_of(lax.rem(first, F), tile)
            lhs = hb[bl, :, :, pl.ds(col, tile)] if F > tile else hb[bl]
            g = dot_tn(lhs.reshape(n * T, tile), grads)
            wg_out[pl.ds(pl.multiple_of(first, tile), tile), :] = g.astype(bf16)
            return acc + jnp.sum(g * g, axis=0, keepdims=True)

        squares = lax.fori_loop(done, done + per, step, squares)
        done += per
        i = turn(s, k, n)
        arrived(g1.at[i], g1_r.at[i])
        for q in range(zpd):
            to = i * zpd + q

            @pl.when(to != z)
            def _():
                pltpu.make_async_remote_copy(
                    src_ref=g1.at[i, q], dst_ref=g2.at[z], send_sem=g2_s.at[s, q], recv_sem=g2_r.at[z],
                    device_id={"dp": k, "vocab": to * cpc + c}, device_id_type=MESH,
                ).start()

            @pl.when(to == z)
            def _():
                pltpu.make_async_copy(g1.at[i, q], g2.at[z], g2_r.at[z]).start()

    total = None
    for src in range(nz):
        arrived(g2.at[src], g2_r.at[src])
        term = g2[src].astype(f32)
        total = term if total is None else total + term
    hg_out[...] = total.astype(bf16)

    both = jnp.sum(squares) + jnp.sum(total * total)
    value = jnp.full((8, 128), both, f32)
    n1s[...] = value
    n1[j] = value
    for s in range(1, nv):
        push(n1s, n1.at[j], n1_s.at[s], n1_r.at[j], k, turn(s, j, nv))
    for s in range(1, nv):
        frm = turn(s, j, nv)
        arrived(n1.at[frm], n1_r.at[frm])
    value = n1[0]
    for a in range(1, nv):
        value = value + n1[a]
    n2s[...] = value
    n2[k] = value
    for s in range(1, n):
        push(n2s, n2.at[k], n2_s.at[s], n2_r.at[k], turn(s, k, n), j)
    for s in range(1, n):
        frm = turn(s, k, n)
        arrived(n2.at[frm], n2_r.at[frm])
    value = n2[0]
    for a in range(1, n):
        value = value + n2[a]
    norm_out[...] = jnp.sqrt(value)

    for src, ss in sends:
        pltpu.make_async_copy(src, src, ss).wait()
    for s in range(n):
        i = turn(s, k, n)
        for q in range(zpd):
            @pl.when(i * zpd + q != z)
            def _():
                pltpu.make_async_copy(g1.at[i, q], g1.at[i, q], g2_s.at[s, q]).wait()


def on_device(n, nv, hidden, weight, targets, loss_mask):
    T, F = hidden.shape
    R, V = weight.shape
    bpd = nv // n
    cpc = 2 if bpd % 2 == 0 else 1
    zpd, nz = bpd // cpc, nv // cpc
    dma = pltpu.SemaphoreType.DMA
    vmem = pl.BlockSpec(memory_space=pltpu.VMEM)
    others = max(cpc - 1, 1)
    hg, wg, loss, norm = pl.pallas_call(
        functools.partial(kernel, n, nv, cpc),
        out_shape=(
            jax.ShapeDtypeStruct((T, F), bf16),
            jax.ShapeDtypeStruct((R, V), bf16),
            jax.ShapeDtypeStruct((1, T), f32),
            jax.ShapeDtypeStruct((8, 128), f32),
        ),
        in_specs=[vmem] * 4,
        out_specs=(vmem,) * 4,
        scratch_shapes=[
            pltpu.VMEM((nz, T, F), bf16),
            pltpu.VMEM((bpd, n, T, F), bf16),
            pltpu.VMEM((n - 1, T, V), f32),
            pltpu.VMEM((n - 1, T, V), f32),
            pltpu.VMEM((8, T), f32),
            pltpu.VMEM((nv, 8, T), f32),
            pltpu.VMEM((n, T, V), bf16),
            pltpu.VMEM((n, others, zpd, T, F), f32),
            pltpu.VMEM((n, others, zpd, T, F), f32),
            pltpu.VMEM((n, zpd, T, F), bf16),
            pltpu.VMEM((n, zpd, T, F), bf16),
            pltpu.VMEM((nz, T, F), bf16),
            pltpu.VMEM((8, 128), f32),
            pltpu.VMEM((nv, 8, 128), f32),
            pltpu.VMEM((8, 128), f32),
            pltpu.VMEM((n, 8, 128), f32),
            dma((nz,)), dma((nz,)),
            dma((n, zpd)), dma((n, bpd)), dma((n, zpd, cpc)),
            dma((n,)), dma((n,)),
            dma((nv,)), dma((nv,)),
            dma((n,)), dma((n,)),
            dma((n, others)), dma((n, others)),
            dma((n,)), dma((n,)),
            dma((n, zpd)), dma((nz,)),
            dma((nv,)), dma((nv,)),
            dma((n,)), dma((n,)),
        ],
        compiler_params=pltpu.CompilerParams(
            collective_id=0, has_side_effects=True, vmem_limit_bytes=60 * 1024 * 1024
        ),
    )(hidden, weight, targets.reshape(1, T), loss_mask.reshape(1, T))
    return hg, wg, loss.reshape(T), norm[0, 0]


def solution(mesh):
    placed = (P("dp", "vocab"), P("dp", "vocab"), P("dp"), P("dp"))
    return jax.shard_map(
        functools.partial(on_device, mesh.shape["dp"], mesh.shape["vocab"]),
        mesh=mesh,
        in_specs=placed,
        out_specs=(P("dp", "vocab"), P("dp", "vocab"), P("dp"), P()),
        check_vma=False,
    )
```

```python
import functools

import jax
import jax.numpy as jnp
from jax import lax
from jax.experimental import pallas as pl
from jax.experimental.pallas import tpu as pltpu
from jax.sharding import PartitionSpec as P

loss_scale = 16.0
MESH = pl.DeviceIdType.MESH
f32 = jnp.float32
bf16 = jnp.bfloat16


def dot_nn(a, b):
    return jnp.dot(a, b, preferred_element_type=f32)


def dot_nt(a, b):
    return lax.dot_general(a, b, (((1,), (1,)), ((), ())), preferred_element_type=f32)


def dot_tn(a, b):
    return lax.dot_general(a, b, (((0,), (0,)), ((), ())), preferred_element_type=f32)


def kernel(
    n, nv, cpc, nc, ng,
    hid, w_in, tgt, keep,
    hg_out, wg_out, loss_out, norm_out,
    w, wg, gat, hb, lp, lr, st, sr, dall, ps, pr, gs, g1, g2, n1s, n1, n2s, n2,
    h1_s, h1_r, h2_s, hb_r, h3_s, l_s, l_r, s_s, s_r, d_s, d_r,
    io, p_s, p_r, g1_s, g1_r, g2_s, g2_r, n1_s, n1_r, n2_s, n2_r,
):
    T, F = hid.shape
    V = w.shape[0]
    Tc, Tg = T // nc, T // ng
    bpd = nv // n
    zpd = bpd // cpc
    nz = nv // cpc
    k = lax.axis_index("dp")
    j = lax.axis_index("vocab")
    z, c = j // cpc, j % cpc
    sends = []

    def push(src, dst, ss, rs, dp, vocab):
        copy = pltpu.make_async_remote_copy(
            src_ref=src, dst_ref=dst, send_sem=ss, recv_sem=rs,
            device_id={"dp": dp, "vocab": vocab}, device_id_type=MESH,
        )
        copy.start()
        sends.append((src, ss))

    def local(src, dst, sem):
        pltpu.make_async_copy(src, dst, sem).start()

    def arrived(dst, sem):
        pltpu.make_async_copy(dst, dst, sem).wait()

    def turn(s, base, size):
        return lax.rem(base + s, size)

    def columns(q, core):
        if F % 128 == 0:
            return w[:, pl.ds(pl.multiple_of((q * cpc + core) * F, F), F)]
        out = w[:, q * cpc * F:(q * cpc + 1) * F]
        for a in range(1, cpc):
            out = jnp.where(core == a, w[:, (q * cpc + a) * F:(q * cpc + a + 1) * F], out)
        return out

    row_order = list(range(1, n)) + [0]

    weight_in = pltpu.make_async_copy(w_in, w, io.at[0])
    weight_in.start()

    barrier = pltpu.get_barrier_semaphore()
    for s in range(1, nv):
        pl.semaphore_signal(barrier, inc=1, device_id={"dp": k, "vocab": turn(s, j, nv)}, device_id_type=MESH)
    for s in range(1, n):
        pl.semaphore_signal(barrier, inc=1, device_id={"dp": turn(s, k, n), "vocab": j}, device_id_type=MESH)
    pl.semaphore_wait(barrier, nv + n - 2)

    for h in range(nc):
        piece = hid.at[pl.ds(h * Tc, Tc)]
        for s in range(1, nz):
            to = turn(s, z, nz)
            push(piece, gat.at[z, h], h1_s.at[s, h], h1_r.at[z, h], k, to * cpc + c)
        local(piece, gat.at[z, h], h1_r.at[z, h])

    def exchange(h):
        for s in row_order:
            i = turn(s, k, n)
            for q in range(zpd):
                src = gat.at[i * zpd + q, h]
                arrived(src, h1_r.at[i * zpd + q, h])
                bl = q * cpc + c
                if s:
                    push(src, hb.at[bl, h, k], h2_s.at[s, q, h], hb_r.at[k, bl, h], i, j)
                else:
                    local(src, hb.at[bl, h, k], hb_r.at[k, bl, h])

    def partial(h):
        for s in [0] + list(range(1, n)):
            t = turn(s, k, n)
            for q in range(zpd):
                bl = q * cpc + c
                slot = hb.at[bl, h, t]
                arrived(slot, hb_r.at[t, bl, h])
                for d in range(1, cpc):
                    push(slot, slot, h3_s.at[s, q, d, h], hb_r.at[t, bl, h], k, z * cpc + turn(d, c, cpc))
        for s in [0] + list(range(1, n)):
            t = turn(s, k, n)
            for q in range(zpd):
                for d in range(1, cpc):
                    bl = q * cpc + turn(d, c, cpc)
                    arrived(hb.at[bl, h, t], hb_r.at[t, bl, h])
        total = dot_nt(hb[0, h].reshape(n * Tc, F), w[:, 0:F])
        for bl in range(1, bpd):
            total += dot_nt(hb[bl, h].reshape(n * Tc, F), w[:, bl * F:(bl + 1) * F])
        lp[h] = total.reshape(n, Tc, V)
        for s in range(1, n):
            t = turn(s, k, n)
            push(lp.at[h, t], lr.at[h, s - 1], l_s.at[s - 1, h], l_r.at[s - 1, h], t, j)

    exchange(0)
    weight_in.wait()
    for h in range(nc):
        if h + 1 < nc:
            exchange(h + 1)
        partial(h)
    rows = []
    for h in range(nc):
        own = lp[h, k]
        for s in range(n - 1):
            arrived(lr.at[h, s], l_r.at[s, h])
            own += lr[h, s]
        rows.append(own)
    logits = jnp.concatenate(rows, axis=0)

    def to_column(row):
        return jnp.transpose(jnp.broadcast_to(row, (128, T)))[:, :1]

    target_col = to_column(tgt[...].astype(f32)).astype(jnp.int32) - j * V
    onehot = lax.broadcasted_iota(jnp.int32, (T, V), 1) == target_col
    top = jnp.max(logits, axis=1, keepdims=True)
    part = jnp.sum(jnp.exp(logits - top), axis=1, keepdims=True)
    hit = jnp.sum(jnp.where(onehot, logits, 0.0), axis=1, keepdims=True)
    lane = lax.broadcasted_iota(jnp.int32, (T, 128), 1)
    packed = jnp.where(lane == 0, top, jnp.where(lane == 1, part, hit))
    mine = jnp.transpose(packed)[:8, :]
    st[...] = mine
    sr[j] = mine
    for s in range(1, nv):
        push(st, sr.at[j], s_s.at[s], s_r.at[j], k, turn(s, j, nv))
    for s in range(1, nv):
        frm = turn(s, j, nv)
        arrived(sr.at[frm], s_r.at[frm])
    stats = sr[...]
    tops, parts, hits = stats[:, 0, :], stats[:, 1, :], stats[:, 2, :]
    row_top = jnp.max(tops, axis=0, keepdims=True)
    exp_sum = jnp.sum(parts * jnp.exp(tops - row_top), axis=0, keepdims=True)
    target_logit = jnp.sum(hits, axis=0, keepdims=True)
    log_total = row_top + jnp.log(exp_sum)
    row_keep = keep[...].astype(f32)
    loss_out[...] = row_keep * (log_total - target_logit)

    soft = jnp.exp(logits - to_column(log_total))
    dl = (loss_scale * to_column(row_keep) * (soft - jnp.where(onehot, 1.0, 0.0))).astype(bf16)
    dall[:, k] = dl.reshape(nc, Tc, V)
    for s in range(1, n):
        push(dall.at[:, k], dall.at[:, k], d_s.at[s], d_r.at[k], turn(s, k, n), j)

    def other_part(s):
        t = turn(s, k, n)
        if s:
            arrived(dall.at[:, t], d_r.at[t])
        rows = dall[:, t].reshape(T, V)
        for d in range(1, cpc):
            other = turn(d, c, cpc)
            for q in range(zpd):
                ps[s, d - 1, q] = dot_nn(rows, columns(q, other))
            push(ps.at[s, d - 1], pr.at[s, d - 1], p_s.at[s, d - 1], p_r.at[s, d - 1], k, z * cpc + other)

    def relay(s, src, q, g):
        to = turn(s, k, n) * zpd + q
        dst = g2.at[z, pl.ds(g * Tg, Tg)]

        @pl.when(to != z)
        def _():
            pltpu.make_async_remote_copy(
                src_ref=src, dst_ref=dst, send_sem=g2_s.at[s, q, g], recv_sem=g2_r.at[z, g],
                device_id={"dp": k, "vocab": to * cpc + c}, device_id_type=MESH,
            ).start()

        @pl.when(to == z)
        def _():
            pltpu.make_async_copy(src, dst, g2_r.at[z, g]).start()

    def own_part(s):
        t = turn(s, k, n)
        rows = dall[:, t].reshape(T, V)
        for d in range(1, cpc):
            arrived(pr.at[s, d - 1], p_r.at[s, d - 1])
        for q in range(zpd):
            part_sum = dot_nn(rows, columns(q, c))
            for d in range(1, cpc):
                part_sum += pr[s, d - 1, q]
            gs[s, q] = part_sum.astype(bf16)
        for g in range(ng):
            if s:
                piece = gs.at[s, :, pl.ds(g * Tg, Tg)]
                push(piece, g1.at[k, :, pl.ds(g * Tg, Tg)], g1_s.at[s, g], g1_r.at[k, g], t, j)
            else:
                for q in range(zpd):
                    relay(0, gs.at[0, q, pl.ds(g * Tg, Tg)], q, g)

    other_part(0)
    own_part(0)
    for s in range(1, n):
        other_part(s)
        if s > 1:
            own_part(s - 1)
    own_part(n - 1)

    grads = jnp.transpose(dall[...].reshape(n * T, V))
    squares = jnp.zeros((1, F), f32)
    per = -(-bpd // n)
    done = 0
    for s in range(1, n + 1):
        for bl in range(done, min(done + per, bpd)):
            grad = dot_nn(grads, hb[bl].reshape(n * T, F))
            wg[:, bl * F:(bl + 1) * F] = grad.astype(bf16)
            squares += jnp.sum(grad * grad, axis=0, keepdims=True)
        done += per
        if s < n:
            i = turn(s, k, n)
            for g in range(ng):
                arrived(g1.at[i, :, pl.ds(g * Tg, Tg)], g1_r.at[i, g])
                for q in range(zpd):
                    relay(s, g1.at[i, q, pl.ds(g * Tg, Tg)], q, g)
    weight_out = pltpu.make_async_copy(wg, wg_out, io.at[1])
    weight_out.start()

    total = None
    for src in range(nz):
        for g in range(ng):
            arrived(g2.at[src, pl.ds(g * Tg, Tg)], g2_r.at[src, g])
        term = g2[src].astype(f32)
        total = term if total is None else total + term
    hg_out[...] = total.astype(bf16)

    both = jnp.sum(squares) + jnp.sum(total * total)
    value = jnp.full((8, 128), both, f32)
    n1s[...] = value
    n1[j] = value
    for s in range(1, nv):
        push(n1s, n1.at[j], n1_s.at[s], n1_r.at[j], k, turn(s, j, nv))
    for s in range(1, nv):
        frm = turn(s, j, nv)
        arrived(n1.at[frm], n1_r.at[frm])
    value = n1[0]
    for a in range(1, nv):
        value = value + n1[a]
    n2s[...] = value
    n2[k] = value
    for s in range(1, n):
        push(n2s, n2.at[k], n2_s.at[s], n2_r.at[k], turn(s, k, n), j)
    for s in range(1, n):
        frm = turn(s, k, n)
        arrived(n2.at[frm], n2_r.at[frm])
    value = n2[0]
    for a in range(1, n):
        value = value + n2[a]
    norm_out[...] = jnp.sqrt(value)

    for src, ss in sends:
        pltpu.make_async_copy(src, src, ss).wait()
    for s in range(n):
        i = turn(s, k, n)
        for q in range(zpd):
            @pl.when(i * zpd + q != z)
            def _():
                for g in range(ng):
                    piece = g2.at[0, pl.ds(0, Tg)]
                    pltpu.make_async_copy(piece, piece, g2_s.at[s, q, g]).wait()
    weight_out.wait()


def on_device(n, nv, hidden, weight, targets, loss_mask):
    T, F = hidden.shape
    R, V = weight.shape
    bpd = nv // n
    cpc = 2 if bpd % 2 == 0 else 1
    zpd, nz = bpd // cpc, nv // cpc
    nc = 4 if T % 64 == 0 else 1
    ng = 2 if T % 32 == 0 else 1
    dma = pltpu.SemaphoreType.DMA
    vmem = pl.BlockSpec(memory_space=pltpu.VMEM)
    hbm = pl.BlockSpec(memory_space=pl.ANY)
    others = max(cpc - 1, 1)
    hg, wg, loss, norm = pl.pallas_call(
        functools.partial(kernel, n, nv, cpc, nc, ng),
        out_shape=(
            jax.ShapeDtypeStruct((T, F), bf16),
            jax.ShapeDtypeStruct((V, R), bf16),
            jax.ShapeDtypeStruct((1, T), f32),
            jax.ShapeDtypeStruct((8, 128), f32),
        ),
        in_specs=[vmem, hbm, vmem, vmem],
        out_specs=(vmem, hbm, vmem, vmem),
        scratch_shapes=[
            pltpu.VMEM((V, R), bf16),
            pltpu.VMEM((V, R), bf16),
            pltpu.VMEM((nz, nc, T // nc, F), bf16),
            pltpu.VMEM((bpd, nc, n, T // nc, F), bf16),
            pltpu.VMEM((nc, n, T // nc, V), f32),
            pltpu.VMEM((nc, n - 1, T // nc, V), f32),
            pltpu.VMEM((8, T), f32),
            pltpu.VMEM((nv, 8, T), f32),
            pltpu.VMEM((nc, n, T // nc, V), bf16),
            pltpu.VMEM((n, others, zpd, T, F), f32),
            pltpu.VMEM((n, others, zpd, T, F), f32),
            pltpu.VMEM((n, zpd, T, F), bf16),
            pltpu.VMEM((n, zpd, T, F), bf16),
            pltpu.VMEM((nz, T, F), bf16),
            pltpu.VMEM((8, 128), f32),
            pltpu.VMEM((nv, 8, 128), f32),
            pltpu.VMEM((8, 128), f32),
            pltpu.VMEM((n, 8, 128), f32),
            dma((nz, nc)), dma((nz, nc)),
            dma((n, zpd, nc)), dma((n, bpd, nc)), dma((n, zpd, cpc, nc)),
            dma((n, nc)), dma((n, nc)),
            dma((nv,)), dma((nv,)),
            dma((n,)), dma((n,)),
            dma((2,)),
            dma((n, others)), dma((n, others)),
            dma((n, ng)), dma((n, ng)),
            dma((n, zpd, ng)), dma((nz, ng)),
            dma((nv,)), dma((nv,)),
            dma((n,)), dma((n,)),
        ],
        compiler_params=pltpu.CompilerParams(
            collective_id=0, has_side_effects=True, vmem_limit_bytes=60 * 1024 * 1024
        ),
    )(hidden, weight.T, targets.reshape(1, T), loss_mask.reshape(1, T))
    return hg, wg.T, loss.reshape(T), norm[0, 0]


def solution(mesh):
    placed = (P("dp", "vocab"), P("dp", "vocab"), P("dp"), P("dp"))
    return jax.shard_map(
        functools.partial(on_device, mesh.shape["dp"], mesh.shape["vocab"]),
        mesh=mesh,
        in_specs=placed,
        out_specs=(P("dp", "vocab"), P("dp", "vocab"), P("dp"), P()),
        check_vma=False,
    )
```

```python
import functools

import jax
import jax.numpy as jnp
from jax import lax
from jax.experimental import pallas as pl
from jax.experimental.pallas import tpu as pltpu
from jax.sharding import PartitionSpec as P

loss_scale = 16.0
MESH = pl.DeviceIdType.MESH
f32 = jnp.float32
bf16 = jnp.bfloat16


def dot_nn(a, b):
    return jnp.dot(a, b, preferred_element_type=f32)


def dot_nt(a, b):
    return lax.dot_general(a, b, (((1,), (1,)), ((), ())), preferred_element_type=f32)


def dot_tn(a, b):
    return lax.dot_general(a, b, (((0,), (0,)), ((), ())), preferred_element_type=f32)


def kernel(
    n, nv, cpc, nc, ng,
    hid, w_in, tgt, keep,
    hg_out, wg_out, loss_out, norm_out,
    w, wg, gat, hb, lp, lr, st, sr, dall, ps, pr, gs, g1, g2, n1s, n1, n2s, n2,
    h1_s, h1_r, h2_s, hb_r, h3_s, l_s, l_r, s_s, s_r, d_s, d_r,
    io, p_s, p_r, g1_s, g1_r, g2_s, g2_r, n1_s, n1_r, n2_s, n2_r,
):
    T, F = hid.shape
    V = w.shape[0]
    Tc, Tg = T // nc, T // ng
    bpd = nv // n
    zpd = bpd // cpc
    nz = nv // cpc
    k = lax.axis_index("dp")
    j = lax.axis_index("vocab")
    z, c = j // cpc, j % cpc
    sends = []

    def push(src, dst, ss, rs, dp, vocab):
        copy = pltpu.make_async_remote_copy(
            src_ref=src, dst_ref=dst, send_sem=ss, recv_sem=rs,
            device_id={"dp": dp, "vocab": vocab}, device_id_type=MESH,
        )
        copy.start()
        sends.append((src, ss))

    def local(src, dst, sem):
        pltpu.make_async_copy(src, dst, sem).start()

    def arrived(dst, sem):
        pltpu.make_async_copy(dst, dst, sem).wait()

    def turn(s, base, size):
        return lax.rem(base + s, size)

    def columns(q, core):
        if F % 128 == 0:
            return w[:, pl.ds(pl.multiple_of((q * cpc + core) * F, F), F)]
        out = w[:, q * cpc * F:(q * cpc + 1) * F]
        for a in range(1, cpc):
            out = jnp.where(core == a, w[:, (q * cpc + a) * F:(q * cpc + a + 1) * F], out)
        return out

    row_order = list(range(1, n)) + [0]

    weight_in = pltpu.make_async_copy(w_in, w, io.at[0])
    weight_in.start()

    barrier = pltpu.get_barrier_semaphore()
    for s in range(1, nv):
        pl.semaphore_signal(barrier, inc=1, device_id={"dp": k, "vocab": turn(s, j, nv)}, device_id_type=MESH)
    for s in range(1, n):
        pl.semaphore_signal(barrier, inc=1, device_id={"dp": turn(s, k, n), "vocab": j}, device_id_type=MESH)
    pl.semaphore_wait(barrier, nv + n - 2)

    for h in range(nc):
        piece = hid.at[pl.ds(h * Tc, Tc)]
        for s in range(1, nz):
            to = turn(s, z, nz)
            push(piece, gat.at[z, h], h1_s.at[s, h], h1_r.at[z, h], k, to * cpc + c)
        local(piece, gat.at[z, h], h1_r.at[z, h])

    def exchange(h):
        for s in row_order:
            i = turn(s, k, n)
            for q in range(zpd):
                src = gat.at[i * zpd + q, h]
                arrived(src, h1_r.at[i * zpd + q, h])
                bl = q * cpc + c
                if s:
                    push(src, hb.at[bl, h, k], h2_s.at[s, q, h], hb_r.at[k, bl, h], i, j)
                else:
                    local(src, hb.at[bl, h, k], hb_r.at[k, bl, h])

    def partial(h):
        for s in [0] + list(range(1, n)):
            t = turn(s, k, n)
            for q in range(zpd):
                bl = q * cpc + c
                slot = hb.at[bl, h, t]
                arrived(slot, hb_r.at[t, bl, h])
                for d in range(1, cpc):
                    push(slot, slot, h3_s.at[s, q, d, h], hb_r.at[t, bl, h], k, z * cpc + turn(d, c, cpc))
        for s in [0] + list(range(1, n)):
            t = turn(s, k, n)
            for q in range(zpd):
                for d in range(1, cpc):
                    bl = q * cpc + turn(d, c, cpc)
                    arrived(hb.at[bl, h, t], hb_r.at[t, bl, h])
        total = dot_nt(hb[0, h].reshape(n * Tc, F), w[:, 0:F])
        for bl in range(1, bpd):
            total += dot_nt(hb[bl, h].reshape(n * Tc, F), w[:, bl * F:(bl + 1) * F])
        lp[h] = total.reshape(n, Tc, V)
        for s in range(1, n):
            t = turn(s, k, n)
            push(lp.at[h, t], lr.at[h, s - 1], l_s.at[s - 1, h], l_r.at[s - 1, h], t, j)

    exchange(0)
    weight_in.wait()
    for h in range(nc):
        if h + 1 < nc:
            exchange(h + 1)
        partial(h)
    rows = []
    for h in range(nc):
        own = lp[h, k]
        for s in range(n - 1):
            arrived(lr.at[h, s], l_r.at[s, h])
            own += lr[h, s]
        rows.append(own)
    logits = jnp.concatenate(rows, axis=0)

    def to_column(row):
        return jnp.transpose(jnp.broadcast_to(row, (128, T)))[:, :1]

    target_col = to_column(tgt[...].astype(f32)).astype(jnp.int32) - j * V
    onehot = lax.broadcasted_iota(jnp.int32, (T, V), 1) == target_col
    top = jnp.max(logits, axis=1, keepdims=True)
    part = jnp.sum(jnp.exp(logits - top), axis=1, keepdims=True)
    hit = jnp.sum(jnp.where(onehot, logits, 0.0), axis=1, keepdims=True)
    lane = lax.broadcasted_iota(jnp.int32, (T, 128), 1)
    packed = jnp.where(lane == 0, top, jnp.where(lane == 1, part, hit))
    mine = jnp.transpose(packed)[:8, :]
    st[...] = mine
    sr[j] = mine
    for s in range(1, nv):
        push(st, sr.at[j], s_s.at[s], s_r.at[j], k, turn(s, j, nv))
    for s in range(1, nv):
        frm = turn(s, j, nv)
        arrived(sr.at[frm], s_r.at[frm])
    stats = sr[...]
    tops, parts, hits = stats[:, 0, :], stats[:, 1, :], stats[:, 2, :]
    row_top = jnp.max(tops, axis=0, keepdims=True)
    exp_sum = jnp.sum(parts * jnp.exp(tops - row_top), axis=0, keepdims=True)
    target_logit = jnp.sum(hits, axis=0, keepdims=True)
    log_total = row_top + jnp.log(exp_sum)
    row_keep = keep[...].astype(f32)
    loss_out[...] = row_keep * (log_total - target_logit)

    soft = jnp.exp(logits - to_column(log_total))
    dl = (loss_scale * to_column(row_keep) * (soft - jnp.where(onehot, 1.0, 0.0))).astype(bf16)
    dall[:, k] = dl.reshape(nc, Tc, V)

    shift = [0] + [1 + lax.rem(z + m, n - 1) for m in range(n - 1)]

    def ahead(s):
        return turn(shift[s], k, n)

    def behind(s):
        return turn(n - shift[s], k, n)

    for s in range(1, n):
        push(dall.at[:, k], dall.at[:, k], d_s.at[s], d_r.at[k], behind(s), j)

    def other_part(s):
        t = ahead(s)
        if s:
            arrived(dall.at[:, t], d_r.at[t])
        rows = dall[:, t].reshape(T, V)
        for d in range(1, cpc):
            other = turn(d, c, cpc)
            for q in range(zpd):
                ps[s, d - 1, q] = dot_nn(rows, columns(q, other))
            push(ps.at[s, d - 1], pr.at[s, d - 1], p_s.at[s, d - 1], p_r.at[s, d - 1], k, z * cpc + other)

    def relay(s, src, q, g):
        to = behind(s) * zpd + q
        dst = g2.at[z, pl.ds(g * Tg, Tg)]

        @pl.when(to != z)
        def _():
            pltpu.make_async_remote_copy(
                src_ref=src, dst_ref=dst, send_sem=g2_s.at[s, q, g], recv_sem=g2_r.at[z, g],
                device_id={"dp": k, "vocab": to * cpc + c}, device_id_type=MESH,
            ).start()

        @pl.when(to == z)
        def _():
            pltpu.make_async_copy(src, dst, g2_r.at[z, g]).start()

    def own_part(s):
        t = ahead(s)
        rows = dall[:, t].reshape(T, V)
        for d in range(1, cpc):
            arrived(pr.at[s, d - 1], p_r.at[s, d - 1])
        for q in range(zpd):
            part_sum = dot_nn(rows, columns(q, c))
            for d in range(1, cpc):
                part_sum += pr[s, d - 1, q]
            gs[s, q] = part_sum.astype(bf16)
        for g in range(ng):
            if s:
                piece = gs.at[s, :, pl.ds(g * Tg, Tg)]
                push(piece, g1.at[k, :, pl.ds(g * Tg, Tg)], g1_s.at[s, g], g1_r.at[k, g], t, j)
            else:
                for q in range(zpd):
                    relay(0, gs.at[0, q, pl.ds(g * Tg, Tg)], q, g)

    other_part(0)
    own_part(0)
    for s in range(1, n):
        other_part(s)
        if s > 1:
            own_part(s - 1)
    own_part(n - 1)

    grads = jnp.transpose(dall[...].reshape(n * T, V))
    squares = jnp.zeros((1, F), f32)
    per = -(-bpd // n)
    done = 0
    for s in range(1, n + 1):
        for bl in range(done, min(done + per, bpd)):
            grad = dot_nn(grads, hb[bl].reshape(n * T, F))
            wg[:, bl * F:(bl + 1) * F] = grad.astype(bf16)
            squares += jnp.sum(grad * grad, axis=0, keepdims=True)
        done += per
        if s < n:
            i = behind(s)
            for g in range(ng):
                arrived(g1.at[i, :, pl.ds(g * Tg, Tg)], g1_r.at[i, g])
                for q in range(zpd):
                    relay(s, g1.at[i, q, pl.ds(g * Tg, Tg)], q, g)
    weight_out = pltpu.make_async_copy(wg, wg_out, io.at[1])
    weight_out.start()

    total = None
    for src in range(nz):
        for g in range(ng):
            arrived(g2.at[src, pl.ds(g * Tg, Tg)], g2_r.at[src, g])
        term = g2[src].astype(f32)
        total = term if total is None else total + term
    hg_out[...] = total.astype(bf16)

    both = jnp.sum(squares) + jnp.sum(total * total)
    value = jnp.full((8, 128), both, f32)
    n1s[...] = value
    n1[j] = value
    for s in range(1, nv):
        push(n1s, n1.at[j], n1_s.at[s], n1_r.at[j], k, turn(s, j, nv))
    for s in range(1, nv):
        frm = turn(s, j, nv)
        arrived(n1.at[frm], n1_r.at[frm])
    value = n1[0]
    for a in range(1, nv):
        value = value + n1[a]
    n2s[...] = value
    n2[k] = value
    for s in range(1, n):
        push(n2s, n2.at[k], n2_s.at[s], n2_r.at[k], turn(s, k, n), j)
    for s in range(1, n):
        frm = turn(s, k, n)
        arrived(n2.at[frm], n2_r.at[frm])
    value = n2[0]
    for a in range(1, n):
        value = value + n2[a]
    norm_out[...] = jnp.sqrt(value)

    for src, ss in sends:
        pltpu.make_async_copy(src, src, ss).wait()
    for s in range(n):
        i = behind(s)
        for q in range(zpd):
            @pl.when(i * zpd + q != z)
            def _():
                for g in range(ng):
                    piece = g2.at[0, pl.ds(0, Tg)]
                    pltpu.make_async_copy(piece, piece, g2_s.at[s, q, g]).wait()
    weight_out.wait()


def on_device(n, nv, hidden, weight, targets, loss_mask):
    T, F = hidden.shape
    R, V = weight.shape
    bpd = nv // n
    cpc = 2 if bpd % 2 == 0 else 1
    zpd, nz = bpd // cpc, nv // cpc
    nc = 4 if T % 64 == 0 else 1
    ng = 2 if T % 32 == 0 else 1
    dma = pltpu.SemaphoreType.DMA
    vmem = pl.BlockSpec(memory_space=pltpu.VMEM)
    hbm = pl.BlockSpec(memory_space=pl.ANY)
    others = max(cpc - 1, 1)
    hg, wg, loss, norm = pl.pallas_call(
        functools.partial(kernel, n, nv, cpc, nc, ng),
        out_shape=(
            jax.ShapeDtypeStruct((T, F), bf16),
            jax.ShapeDtypeStruct((V, R), bf16),
            jax.ShapeDtypeStruct((1, T), f32),
            jax.ShapeDtypeStruct((8, 128), f32),
        ),
        in_specs=[vmem, hbm, vmem, vmem],
        out_specs=(vmem, hbm, vmem, vmem),
        scratch_shapes=[
            pltpu.VMEM((V, R), bf16),
            pltpu.VMEM((V, R), bf16),
            pltpu.VMEM((nz, nc, T // nc, F), bf16),
            pltpu.VMEM((bpd, nc, n, T // nc, F), bf16),
            pltpu.VMEM((nc, n, T // nc, V), f32),
            pltpu.VMEM((nc, n - 1, T // nc, V), f32),
            pltpu.VMEM((8, T), f32),
            pltpu.VMEM((nv, 8, T), f32),
            pltpu.VMEM((nc, n, T // nc, V), bf16),
            pltpu.VMEM((n, others, zpd, T, F), f32),
            pltpu.VMEM((n, others, zpd, T, F), f32),
            pltpu.VMEM((n, zpd, T, F), bf16),
            pltpu.VMEM((n, zpd, T, F), bf16),
            pltpu.VMEM((nz, T, F), bf16),
            pltpu.VMEM((8, 128), f32),
            pltpu.VMEM((nv, 8, 128), f32),
            pltpu.VMEM((8, 128), f32),
            pltpu.VMEM((n, 8, 128), f32),
            dma((nz, nc)), dma((nz, nc)),
            dma((n, zpd, nc)), dma((n, bpd, nc)), dma((n, zpd, cpc, nc)),
            dma((n, nc)), dma((n, nc)),
            dma((nv,)), dma((nv,)),
            dma((n,)), dma((n,)),
            dma((2,)),
            dma((n, others)), dma((n, others)),
            dma((n, ng)), dma((n, ng)),
            dma((n, zpd, ng)), dma((nz, ng)),
            dma((nv,)), dma((nv,)),
            dma((n,)), dma((n,)),
        ],
        compiler_params=pltpu.CompilerParams(
            collective_id=0, has_side_effects=True, vmem_limit_bytes=60 * 1024 * 1024
        ),
    )(hidden, weight.T, targets.reshape(1, T), loss_mask.reshape(1, T))
    return hg, wg.T, loss.reshape(T), norm[0, 0]


def solution(mesh):
    placed = (P("dp", "vocab"), P("dp", "vocab"), P("dp"), P("dp"))
    return jax.shard_map(
        functools.partial(on_device, mesh.shape["dp"], mesh.shape["vocab"]),
        mesh=mesh,
        in_specs=placed,
        out_specs=(P("dp", "vocab"), P("dp", "vocab"), P("dp"), P()),
        check_vma=False,
    )
```
